32 devices in a mesh: grid: 8 (over y, x, core), band: 4 (over z).
Axes of the slice: x: 2, y: 2, z: 4, core: 2. Of those that a mesh axis runs over, the one named last changes fastest.
Arguments:
- start: float32 [1, 4, 1, 64, 32768], P(None, None, None, 'band', 'grid'), may hold values from -6 to 6
- energies: float32 [4, 64, 32768], P(None, 'band', 'grid'), may hold values from -4 to 4
- sites: int32 [3, 1], replicated, may hold values from 0 to 31
- potential: float32 [32, 32, 32], replicated, may hold values from -4 to 400
Outputs:
- alphas: float32 [1, 1, 4], replicated
- betas: float32 [1, 1, 4], replicated
- lanczos: float32 [1, 4, 1, 64, 32768], P(None, None, None, 'band', 'grid')
The draws below stay inside these ranges and needn't reach their ends.
All inputs are finite; a program needn't handle non-finite values.
Results may differ from the reference program's by a relative error of at most 0.0003.
Values sent between devices are 32-bit elements; how exact they have to be, the bound alone decides.
A program may use at most 64 MiB of HBM per device.

```python
import jax
import jax.numpy as jnp
from jax import lax

GRIDN = 32
CBANDS = 64
CORES = 4
POLS = 1
ITERS = 4
ATOMS = 1
KPOINTS = 32768


def draw_potential(key, part):
    first, second = jax.random.split(key)
    coords = jnp.arange(GRIDN, dtype=jnp.int32)
    distance = jnp.minimum(coords, GRIDN - coords).astype(jnp.float32)
    square = distance[:, None, None] ** 2 + distance[None, :, None] ** 2 + distance[None, None, :] ** 2
    radius = jnp.sqrt(square)
    spread_cells, height, tail_charge, background = (1.5, 250.0, 6.0, 3.0)
    roughness = jax.random.uniform(first, (GRIDN, GRIDN, GRIDN), jnp.float32, 0.5, 1.5)
    jitter = jax.random.uniform(second, (GRIDN, GRIDN, GRIDN), jnp.float32, -1.0, 1.0)
    peaked = height * jnp.exp(-square / (2.0 * spread_cells * spread_cells)) * roughness
    screened_tail = tail_charge / jnp.maximum(radius, 0.5)
    return peaked + screened_tail + background * jitter


def block_scale(rng, extent, shards, least, top_value):
    def one(position, parts):
        steps = jax.random.uniform(jax.random.fold_in(jax.random.fold_in(rng, 6), position), (parts,), jnp.float32, least / len(shards), top_value / len(shards))
        return jnp.repeat(jnp.exp(steps), extent[position] // parts).reshape((-1,) + (1,) * (len(extent) - position - 1))

    gain = one(*shards[0])
    for cut in shards[1:]:
        gain = gain * one(*cut)
    return gain


def scatter_about(key, extent, spread, reach, pieces=(), kind=jnp.bfloat16):
    array = spread * jax.random.normal(key, extent, jnp.float32)
    if pieces:
        array = array * block_scale(key, extent, pieces, -0.22, 0.18)
    return jnp.clip(array, -reach, reach).astype(kind)


def setup_inputs(seed: int = 0) -> dict:
    splits = jax.random.split(jax.random.key(seed), 5)
    start = scatter_about(splits[0], (ATOMS, CORES, POLS, CBANDS, KPOINTS), 1.0, 6.0, ((3, 4), (4, 8)), jnp.float32)
    energies = jnp.clip(jax.random.uniform(splits[1], (CORES, CBANDS, KPOINTS), jnp.float32, -4.0, 4.0) * block_scale(splits[1], (CORES, CBANDS, KPOINTS), ((1, 4), (2, 8)), -0.4, 0.0), -4.0, 4.0)
    sites = jax.random.randint(splits[2], (3, ATOMS), 0, GRIDN).astype(jnp.int32)
    potential = draw_potential(jax.random.fold_in(splits[4], 71), 0)
    return dict(start=start, energies=energies, sites=sites, potential=potential)


def cas_along(field_part, axis_number):
    spectrum = jnp.fft.fft(field_part, axis=axis_number)
    return (spectrum.real - spectrum.imag).astype(field_part.dtype)

def cas_three(field_part):
    return cas_along(cas_along(cas_along(field_part, 1), 2), 3)

def shift_axis(field_part, offset, axis_number):
    length = field_part.shape[axis_number]
    doubled = jnp.concatenate([field_part, field_part], axis=axis_number)
    first_index = ((length - offset) % length).astype(jnp.int32)
    return lax.dynamic_slice_in_dim(doubled, first_index, length, axis_number)

def reference(start, energies, sites, potential):
    grid_size = potential.shape[0]
    volume = grid_size * grid_size * grid_size
    shifted_list = []
    for atom_index in range(ATOMS):
        shifted = shift_axis(potential, sites[0, atom_index], 0)
        shifted = shift_axis(shifted, sites[1, atom_index], 1)
        shifted = shift_axis(shifted, sites[2, atom_index], 2)
        shifted_list.append(shifted)
    weights_all = jnp.repeat(jnp.stack(shifted_list), CORES, axis=0)

    def per_block(pair_items):
        field_block, weights = pair_items
        return cas_three(weights[None] * cas_three(field_block)) / volume

    def direct(vector):
        flat_vec = vector.reshape(ATOMS * CORES, POLS * CBANDS, grid_size, grid_size, grid_size)
        result = lax.map(per_block, (flat_vec, weights_all))
        return result.reshape(vector.shape)
    total_count = CORES * CBANDS * KPOINTS

    def inner(left, right):
        return lax.optimization_barrier(jnp.sum(left * right, axis=(1, 3, 4))) / total_count

    def expand_coef(values):
        return values[:, None, :, None, None]
    lanczos = start / expand_coef(jnp.sqrt(inner(start, start)))
    previous = jnp.zeros_like(start)
    beta_prev = jnp.zeros((ATOMS, POLS), jnp.float32)
    alpha_list = []
    beta_list = []
    for iteration in range(ITERS):
        applied = energies[None, :, None] * lanczos - direct(lanczos)
        alpha_now = inner(lanczos, applied)
        remainder = applied - expand_coef(alpha_now) * lanczos - expand_coef(beta_prev) * previous
        beta_now = jnp.sqrt(inner(remainder, remainder))
        previous = lanczos
        lanczos = remainder / expand_coef(beta_now)
        beta_prev = beta_now
        alpha_list.append(alpha_now)
        beta_list.append(beta_now)
    return (jnp.stack(alpha_list, axis=2), jnp.stack(beta_list, axis=2), lanczos)
```

```python
import functools
import math

import jax
import jax.numpy as jnp
import numpy as np
from jax import lax
from jax.experimental import pallas as pl
from jax.experimental.pallas import tpu as pltpu
from jax.sharding import PartitionSpec as P

ITERS = 4


precise_mode = lax.Precision.HIGHEST


def cas_table(grid_size):
    cells = jnp.arange(grid_size, dtype=jnp.int32)
    phase = cells[:, None] * cells[None, :] % grid_size
    angle = phase.astype(jnp.float32) * (2.0 * math.pi / grid_size)
    return jnp.cos(angle) + jnp.sin(angle)


def shift_axis(field_part, offset, axis_number):
    length = field_part.shape[axis_number]
    doubled = jnp.concatenate([field_part, field_part], axis=axis_number)
    first_index = (length - offset) % length
    return lax.dynamic_slice_in_dim(doubled, first_index, length, axis_number)


def expand_coef(values):
    return values[:, None, :, None, None]


def plane_body(start, energies, sites, potential):
    grid_size = potential.shape[0]
    volume = grid_size * grid_size * grid_size
    atom_count, core_count, pol_count, band_local, kpoint_local = start.shape
    plane_count = grid_size // lax.axis_size("grid")
    position = lax.axis_index("grid")
    chain_count = core_count * pol_count * band_local
    field_count = atom_count * chain_count
    total_count = (
        core_count * band_local * lax.axis_size("band") * kpoint_local * lax.axis_size("grid")
    )
    cas_grid = cas_table(grid_size)
    shifted = shift_axis(potential, sites[0, 0], 0)
    shifted = shift_axis(shifted, sites[1, 0], 1)
    shifted = shift_axis(shifted, sites[2, 0], 2)
    tables = [shifted]
    shifted_all = jnp.stack(tables, axis=-1)
    slab_table = lax.dynamic_slice_in_dim(shifted_all, position * plane_count, plane_count, 1)

    def moment(left, right):
        return jnp.sum(left * right, axis=(1, 3, 4)) / total_count

    start_sum = lax.psum(moment(start, start), ("grid", "band"))
    lanczos = start / expand_coef(jnp.sqrt(start_sum))
    previous = jnp.zeros_like(start)
    beta_prev = jnp.zeros((atom_count, pol_count), jnp.float32)
    alpha_list = []
    beta_list = []
    for iteration in range(ITERS):
        spread_fields = lanczos.reshape(atom_count, chain_count, plane_count, grid_size, grid_size)
        spread_over_z = jnp.einsum(
            "arpyz,wz->pywar", spread_fields, cas_grid, precision=precise_mode
        )
        spread_over_y = jnp.einsum(
            "pywar,uy->puwar", spread_over_z, cas_grid, precision=precise_mode
        )
        direct_spectrum = lax.all_to_all(
            spread_over_y.reshape(plane_count, grid_size, grid_size, field_count),
            "grid",
            split_axis=1,
            concat_axis=0,
            tiled=True,
        )
        field_shape = direct_spectrum.shape
        over_x = jnp.einsum("xvwf,tx->tvwf", direct_spectrum, cas_grid, precision=precise_mode)
        split_view = over_x.reshape(
            field_shape[0], field_shape[1], field_shape[2], atom_count, chain_count
        )
        scaled = split_view * slab_table[..., None]
        back_x = jnp.einsum("tvwar,xt->xvwar", scaled, cas_grid, precision=precise_mode)
        weighted = back_x.reshape(field_shape)
        direct_returned = lax.all_to_all(weighted, "grid", split_axis=0, concat_axis=1, tiled=True)
        fields = direct_returned.reshape(plane_count, grid_size, grid_size, atom_count, chain_count)
        over_z = jnp.einsum("pvwar,zw->pvzar", fields, cas_grid, precision=precise_mode)
        over_y = jnp.einsum("pvzar,yv->arpyz", over_z, cas_grid, precision=precise_mode)
        applied = energies[None, :, None] * lanczos - over_y.reshape(start.shape) / volume
        moments_all = lax.psum(
            (
                moment(lanczos, applied),
                moment(applied, applied),
                moment(lanczos, lanczos),
                moment(previous, previous),
                moment(previous, applied),
                moment(lanczos, previous),
            ),
            ("grid", "band"),
        )
        alpha_now = moments_all[0]
        square = (
            moments_all[1]
            + alpha_now * alpha_now * moments_all[2]
            + beta_prev * beta_prev * moments_all[3]
        )
        square = square - 2.0 * alpha_now * moments_all[0] - 2.0 * beta_prev * moments_all[4]
        square = square + 2.0 * alpha_now * beta_prev * moments_all[5]
        beta_now = jnp.sqrt(square)
        remainder = applied - expand_coef(alpha_now) * lanczos - expand_coef(beta_prev) * previous
        previous = lanczos
        lanczos = remainder / expand_coef(beta_now)
        beta_prev = beta_now
        alpha_list.append(alpha_now)
        beta_list.append(beta_now)
    return (jnp.stack(alpha_list, axis=2), jnp.stack(beta_list, axis=2), lanczos)


MESH = pl.DeviceIdType.MESH
LANES = 128
SUBLANES = 8


def split(value):
    high = value.astype(jnp.bfloat16)
    return high, (value - high.astype(jnp.float32)).astype(jnp.bfloat16)


def dot3(left, right):
    left_high, left_low = left
    right_high, right_low = right
    total = jnp.dot(left_high, right_high, preferred_element_type=jnp.float32)
    total += jnp.dot(left_low, right_high, preferred_element_type=jnp.float32)
    return total + jnp.dot(left_high, right_low, preferred_element_type=jnp.float32)


def shifted_potential(table, sites, grid_size):
    cells = grid_size * grid_size
    lane = lax.broadcasted_iota(jnp.int32, table.shape, 1) % grid_size
    for axis in range(3):
        step = 1
        while step < grid_size:
            if axis == 0:
                moved = pltpu.roll(table, step, 0)
            elif axis == 1:
                moved = pltpu.roll(table, step * grid_size, 1)
            else:
                moved = jnp.where(
                    lane >= step,
                    pltpu.roll(table, step, 1),
                    pltpu.roll(table, cells - grid_size + step, 1),
                )
            flag = jnp.full(table.shape, sites[axis, 0] // step % 2, jnp.int32)
            table = jnp.where(flag == 1, moved, table)
            step *= 2
    return table


def recursion_kernel(
    sizes, start, energies, sites, pot, y_table, z_table, x_high, x_low,
    out, coef,
    got, got_energies, vec, prev, applied, energy, site_table, vec_high, vec_low,
    mid_high, mid_low, mat_high, mat_low, outgoing, grid_sums, band_sums,
    start_send, start_recv, energy_send, energy_recv, out_send, out_recv,
    grid_send, grid_recv, band_send, band_recv,
):
    n, band_n, grid_size, halves, block = sizes
    me = lax.axis_index("grid")
    band_me = lax.axis_index("band")
    cells = grid_size * grid_size
    planes = grid_size // n
    rows = grid_size * SUBLANES
    total_count = float(rows * cells * n * band_n)

    barrier = pltpu.get_barrier_semaphore()
    for k in range(1, n):
        pl.semaphore_signal(barrier, inc=1, device_id={"grid": (me + k) % n}, device_id_type=MESH)
    for k in range(1, band_n):
        pl.semaphore_signal(barrier, inc=1, device_id={"band": (band_me + k) % band_n}, device_id_type=MESH)
    pl.semaphore_wait(barrier, n + band_n - 2)

    def start_piece(owner):
        return start.at[0, owner // halves, 0, pl.ds(pl.multiple_of(owner % halves * SUBLANES, SUBLANES), SUBLANES), :]

    def energy_piece(owner):
        return energies.at[owner // halves, pl.ds(pl.multiple_of(owner % halves * SUBLANES, SUBLANES), SUBLANES), :]

    def out_piece(owner):
        return out.at[0, owner // halves, 0, pl.ds(pl.multiple_of(owner % halves * SUBLANES, SUBLANES), SUBLANES), :]

    def spread(piece, landing, send, recv):
        copies = []
        for k in range(1, n):
            peer = (me + k) % n
            copies.append(pltpu.make_async_remote_copy(
                src_ref=piece(peer), dst_ref=landing.at[me], send_sem=send.at[k], recv_sem=recv.at[k],
                device_id={"grid": peer}, device_id_type=MESH))
        own = pltpu.make_async_copy(piece(me), landing.at[me], send.at[0])
        for copy in copies:
            copy.start()
        own.start()
        return copies + [own]

    start_copies = spread(start_piece, got, start_send, start_recv)
    energy_copies = spread(energy_piece, got_energies, energy_send, energy_recv)

    def matrix_rows(y, carry):
        high, low = split(y_table[pl.ds(y, 1), :] * z_table[...])
        at = pl.ds(pl.multiple_of(y * grid_size, grid_size), grid_size)
        mat_high[at, :] = high
        mat_low[at, :] = low
        return carry

    lax.fori_loop(0, grid_size, matrix_rows, 0)
    table = shifted_potential(pot[...], sites, grid_size) * (1.0 / (grid_size * cells))
    for x in range(grid_size):
        site_table[SUBLANES * x:SUBLANES * (x + 1), :] = jnp.broadcast_to(table[x:x + 1, :], (SUBLANES, cells))
    prev[...] = jnp.zeros_like(prev)

    for copy in start_copies:
        copy.wait()
    for x in range(grid_size):
        at = slice(SUBLANES * x, SUBLANES * (x + 1))
        vec[at, :] = got[x // planes, :, x % planes * cells:(x % planes + 1) * cells]
    vec_high[...], vec_low[...] = split(vec[...])

    blocks = [slice(i, i + block) for i in range(0, cells, block)]
    lane = lax.broadcasted_iota(jnp.int32, (1, LANES), 1)

    def step(j, carry):
        alphas, betas, beta_prev = carry
        x_pair = (x_high[...], x_low[...])
        for cols in blocks:
            mat = (mat_high[:, cols], mat_low[:, cols])
            spectrum = dot3((vec_high[...], vec_low[...]), mat)
            spectrum = dot3(x_pair, split(spectrum)) * site_table[:, cols]
            mid_high[:, cols], mid_low[:, cols] = split(dot3(x_pair, split(spectrum)))

        @pl.when(j == 0)
        def _():
            for copy in energy_copies:
                copy.wait()
            for x in range(grid_size):
                at = slice(SUBLANES * x, SUBLANES * (x + 1))
                energy[at, :] = got_energies[x // planes, :, x % planes * cells:(x % planes + 1) * cells]

        sums = [jnp.zeros((1, block), jnp.float32)] * 6
        for cols in blocks:
            mat = (mat_high[:, cols], mat_low[:, cols])
            here, before = vec[:, cols], prev[:, cols]
            new = energy[:, cols] * here - dot3((mid_high[...], mid_low[...]), mat)
            applied[:, cols] = new
            for i, (a, b) in enumerate(((here, new), (new, new), (here, here), (before, before), (before, new), (here, before))):
                sums[i] = sums[i] + jnp.sum(a * b, axis=0, keepdims=True)
        message = jnp.zeros((1, LANES), jnp.float32)
        for i in range(6):
            message = jnp.where(lane == i, jnp.sum(sums[i], axis=1, keepdims=True), message)

        def total(message, buffer, axis, size, my, send, recv):
            buffer[j, my] = message
            copies = []
            for k in range(1, size):
                copy = pltpu.make_async_remote_copy(
                    src_ref=buffer.at[j, my], dst_ref=buffer.at[j, my], send_sem=send.at[j, k], recv_sem=recv.at[j, k],
                    device_id={axis: (my + k) % size}, device_id_type=MESH)
                copy.start()
                copies.append(copy)
            for copy in copies:
                copy.wait()
            return jnp.sum(buffer[j], axis=0)

        message = total(message, grid_sums, "grid", n, me, grid_send, grid_recv)
        message = total(message, band_sums, "band", band_n, band_me, band_send, band_recv)
        m = [jnp.sum(jnp.where(lane == i, message, 0.0), axis=1, keepdims=True) / total_count for i in range(6)]
        norm = jnp.where(jnp.full((1, 1), j, jnp.int32) == 0, m[2], 1.0)
        scale = jnp.sqrt(norm)
        alpha = m[0] / norm
        square = m[1] / norm + alpha * alpha * (m[2] / norm) + beta_prev * beta_prev * m[3]
        square = square - 2.0 * alpha * alpha - 2.0 * beta_prev * m[4]
        square = square + 2.0 * alpha * beta_prev * m[5]
        beta = jnp.sqrt(square)
        to_new = 1.0 / (scale * beta)
        to_here = alpha * to_new
        to_before = beta_prev / beta
        to_prev = 1.0 / scale
        for x in range(0, grid_size, planes):
            at = slice(SUBLANES * x, SUBLANES * (x + planes))
            here = vec[at, :]
            value = to_new * applied[at, :] - to_here * here - to_before * prev[at, :]
            prev[at, :] = to_prev * here
            vec[at, :] = value
            vec_high[at, :], vec_low[at, :] = split(value)
        alphas = jnp.where(lane == j, alpha, alphas)
        betas = jnp.where(lane == j, beta, betas)
        return alphas, betas, beta

    zeros = jnp.zeros((1, LANES), jnp.float32)
    alphas, betas, _ = lax.fori_loop(0, ITERS, step, (zeros, zeros, jnp.zeros((1, 1), jnp.float32)))
    coef[0:1, :] = alphas
    coef[1:2, :] = betas
    for x in range(grid_size):
        at = slice(SUBLANES * x, SUBLANES * (x + 1))
        outgoing[x // planes, :, x % planes * cells:(x % planes + 1) * cells] = vec[at, :]
    out_copies = []
    for k in range(1, n):
        peer = (me + k) % n
        out_copies.append(pltpu.make_async_remote_copy(
            src_ref=outgoing.at[peer], dst_ref=out_piece(me), send_sem=out_send.at[k], recv_sem=out_recv.at[k],
            device_id={"grid": peer}, device_id_type=MESH))
    out_copies.append(pltpu.make_async_copy(outgoing.at[me], out_piece(me), out_send.at[0]))
    for copy in out_copies:
        copy.start()
    for copy in out_copies:
        copy.wait()


def field_body(start, energies, sites, potential):
    grid_size = potential.shape[0]
    cells = grid_size * grid_size
    n, band_n = lax.axis_size("grid"), lax.axis_size("band")
    halves = start.shape[3] // SUBLANES
    rows = grid_size * SUBLANES
    index = np.arange(grid_size)
    angle = (index[:, None] * index[None, :] % grid_size) * (2.0 * math.pi / grid_size)
    cas = np.cos(angle) + np.sin(angle)
    y_table = jnp.asarray(np.repeat(cas, grid_size, axis=1), jnp.float32)
    z_table = jnp.asarray(np.tile(cas, (1, grid_size)), jnp.float32)
    x_wide = np.kron(cas, np.eye(SUBLANES)).astype(np.float32)
    x_high = x_wide.astype(jnp.bfloat16)
    x_low = (x_wide - x_high.astype(np.float32)).astype(jnp.bfloat16)
    vmem = pl.BlockSpec(memory_space=pltpu.VMEM)
    hbm = pl.BlockSpec(memory_space=pl.ANY)
    slab = (n, SUBLANES, start.shape[4])
    full = pltpu.VMEM((rows, cells), jnp.float32)
    half = pltpu.VMEM((rows, cells), jnp.bfloat16)
    dma = pltpu.SemaphoreType.DMA
    out, coef = pl.pallas_call(
        functools.partial(recursion_kernel, (n, band_n, grid_size, halves, min(256, cells))),
        out_shape=(jax.ShapeDtypeStruct(start.shape, jnp.float32), jax.ShapeDtypeStruct((2, LANES), jnp.float32)),
        in_specs=[hbm, hbm, pl.BlockSpec(memory_space=pltpu.SMEM)] + [vmem] * 5,
        out_specs=(hbm, vmem),
        scratch_shapes=[
            pltpu.VMEM(slab, jnp.float32), pltpu.VMEM(slab, jnp.float32),
            full, full, full, full, full, half, half, half, half,
            pltpu.VMEM((cells, cells), jnp.bfloat16), pltpu.VMEM((cells, cells), jnp.bfloat16),
            pltpu.VMEM(slab, jnp.float32),
            pltpu.VMEM((ITERS, n, 1, LANES), jnp.float32), pltpu.VMEM((ITERS, band_n, 1, LANES), jnp.float32),
            dma((n,)), dma((n,)), dma((n,)), dma((n,)), dma((n,)), dma((n,)),
            dma((ITERS, n)), dma((ITERS, n)), dma((ITERS, band_n)), dma((ITERS, band_n)),
        ],
        compiler_params=pltpu.CompilerParams(collective_id=0, has_side_effects=True, vmem_limit_bytes=50 * 1024 * 1024),
    )(start, energies, sites, potential.reshape(grid_size, cells), y_table, z_table, jnp.asarray(x_high), jnp.asarray(x_low))
    return coef[0, :ITERS].reshape(1, 1, ITERS), coef[1, :ITERS].reshape(1, 1, ITERS), out


def body(start, energies, sites, potential):
    atoms, cores, pols, bands, _ = start.shape
    grid_size = potential.shape[0]
    whole_fields = (
        atoms == 1 and pols == 1 and bands % SUBLANES == 0
        and cores * bands == SUBLANES * lax.axis_size("grid")
        and grid_size % SUBLANES == 0 and grid_size * grid_size % LANES == 0
    )
    return (field_body if whole_fields else plane_body)(start, energies, sites, potential)


def solution(mesh):
    in_specs = (P(None, None, None, "band", "grid"), P(None, "band", "grid"), P(), P())
    out_specs = (P(), P(), P(None, None, None, "band", "grid"))
    return jax.shard_map(body, mesh=mesh, in_specs=in_specs, out_specs=out_specs, check_vma=False)
```

```python
import functools
import math

import jax
import jax.numpy as jnp
import numpy as np
from jax import lax
from jax.experimental import pallas as pl
from jax.experimental.pallas import tpu as pltpu
from jax.sharding import PartitionSpec as P

ITERS = 4


precise_mode = lax.Precision.HIGHEST


def cas_table(grid_size):
    cells = jnp.arange(grid_size, dtype=jnp.int32)
    phase = cells[:, None] * cells[None, :] % grid_size
    angle = phase.astype(jnp.float32) * (2.0 * math.pi / grid_size)
    return jnp.cos(angle) + jnp.sin(angle)


def shift_axis(field_part, offset, axis_number):
    length = field_part.shape[axis_number]
    doubled = jnp.concatenate([field_part, field_part], axis=axis_number)
    first_index = (length - offset) % length
    return lax.dynamic_slice_in_dim(doubled, first_index, length, axis_number)


def expand_coef(values):
    return values[:, None, :, None, None]


def plane_body(start, energies, sites, potential):
    grid_size = potential.shape[0]
    volume = grid_size * grid_size * grid_size
    atom_count, core_count, pol_count, band_local, kpoint_local = start.shape
    plane_count = grid_size // lax.axis_size("grid")
    position = lax.axis_index("grid")
    chain_count = core_count * pol_count * band_local
    field_count = atom_count * chain_count
    total_count = (
        core_count * band_local * lax.axis_size("band") * kpoint_local * lax.axis_size("grid")
    )
    cas_grid = cas_table(grid_size)
    shifted = shift_axis(potential, sites[0, 0], 0)
    shifted = shift_axis(shifted, sites[1, 0], 1)
    shifted = shift_axis(shifted, sites[2, 0], 2)
    tables = [shifted]
    shifted_all = jnp.stack(tables, axis=-1)
    slab_table = lax.dynamic_slice_in_dim(shifted_all, position * plane_count, plane_count, 1)

    def moment(left, right):
        return jnp.sum(left * right, axis=(1, 3, 4)) / total_count

    start_sum = lax.psum(moment(start, start), ("grid", "band"))
    lanczos = start / expand_coef(jnp.sqrt(start_sum))
    previous = jnp.zeros_like(start)
    beta_prev = jnp.zeros((atom_count, pol_count), jnp.float32)
    alpha_list = []
    beta_list = []
    for iteration in range(ITERS):
        spread_fields = lanczos.reshape(atom_count, chain_count, plane_count, grid_size, grid_size)
        spread_over_z = jnp.einsum(
            "arpyz,wz->pywar", spread_fields, cas_grid, precision=precise_mode
        )
        spread_over_y = jnp.einsum(
            "pywar,uy->puwar", spread_over_z, cas_grid, precision=precise_mode
        )
        direct_spectrum = lax.all_to_all(
            spread_over_y.reshape(plane_count, grid_size, grid_size, field_count),
            "grid",
            split_axis=1,
            concat_axis=0,
            tiled=True,
        )
        field_shape = direct_spectrum.shape
        over_x = jnp.einsum("xvwf,tx->tvwf", direct_spectrum, cas_grid, precision=precise_mode)
        split_view = over_x.reshape(
            field_shape[0], field_shape[1], field_shape[2], atom_count, chain_count
        )
        scaled = split_view * slab_table[..., None]
        back_x = jnp.einsum("tvwar,xt->xvwar", scaled, cas_grid, precision=precise_mode)
        weighted = back_x.reshape(field_shape)
        direct_returned = lax.all_to_all(weighted, "grid", split_axis=0, concat_axis=1, tiled=True)
        fields = direct_returned.reshape(plane_count, grid_size, grid_size, atom_count, chain_count)
        over_z = jnp.einsum("pvwar,zw->pvzar", fields, cas_grid, precision=precise_mode)
        over_y = jnp.einsum("pvzar,yv->arpyz", over_z, cas_grid, precision=precise_mode)
        applied = energies[None, :, None] * lanczos - over_y.reshape(start.shape) / volume
        moments_all = lax.psum(
            (
                moment(lanczos, applied),
                moment(applied, applied),
                moment(lanczos, lanczos),
                moment(previous, previous),
                moment(previous, applied),
                moment(lanczos, previous),
            ),
            ("grid", "band"),
        )
        alpha_now = moments_all[0]
        square = (
            moments_all[1]
            + alpha_now * alpha_now * moments_all[2]
            + beta_prev * beta_prev * moments_all[3]
        )
        square = square - 2.0 * alpha_now * moments_all[0] - 2.0 * beta_prev * moments_all[4]
        square = square + 2.0 * alpha_now * beta_prev * moments_all[5]
        beta_now = jnp.sqrt(square)
        remainder = applied - expand_coef(alpha_now) * lanczos - expand_coef(beta_prev) * previous
        previous = lanczos
        lanczos = remainder / expand_coef(beta_now)
        beta_prev = beta_now
        alpha_list.append(alpha_now)
        beta_list.append(beta_now)
    return (jnp.stack(alpha_list, axis=2), jnp.stack(beta_list, axis=2), lanczos)


MESH = pl.DeviceIdType.MESH
LANES = 128
SUBLANES = 8


def split(value):
    high = value.astype(jnp.bfloat16)
    return high, (value - high.astype(jnp.float32)).astype(jnp.bfloat16)


def dot3(left, right):
    left_high, left_low = left
    right_high, right_low = right
    total = jnp.dot(left_high, right_high, preferred_element_type=jnp.float32)
    total += jnp.dot(left_low, right_high, preferred_element_type=jnp.float32)
    return total + jnp.dot(left_high, right_low, preferred_element_type=jnp.float32)


def shifted_potential(table, sites, grid_size):
    cells = grid_size * grid_size
    lane = lax.broadcasted_iota(jnp.int32, table.shape, 1) % grid_size
    for axis in range(3):
        step = 1
        while step < grid_size:
            if axis == 0:
                moved = pltpu.roll(table, step, 0)
            elif axis == 1:
                moved = pltpu.roll(table, step * grid_size, 1)
            else:
                moved = jnp.where(
                    lane >= step,
                    pltpu.roll(table, step, 1),
                    pltpu.roll(table, cells - grid_size + step, 1),
                )
            flag = jnp.full(table.shape, sites[axis] // step % 2, jnp.int32)
            table = jnp.where(flag == 1, moved, table)
            step *= 2
    return table


def recursion_kernel(
    sizes, start, energies, sites, pot, y_table, z_table, x_high, x_low,
    out, alphas_out, betas_out,
    pot_here, pot_flat, got, got_energies, vec, prev, applied, applied_prev, twice, energy, site_table, vec_high, vec_low,
    mid_high, mid_low, mat_high, mat_low, outgoing, grid_sums, band_sums,
    pot_sem, start_send, start_recv, energy_send, energy_recv, out_send, out_recv,
    grid_send, grid_recv, band_send, band_recv,
):
    n, band_n, grid_size, halves, block = sizes
    me = lax.axis_index("grid")
    band_me = lax.axis_index("band")
    cells = grid_size * grid_size
    planes = grid_size // n
    rows = grid_size * SUBLANES
    total_count = float(rows * cells * n * band_n)

    pot_copy = pltpu.make_async_copy(pot, pot_here, pot_sem)
    pot_copy.start()
    barrier = pltpu.get_barrier_semaphore()
    for k in range(1, n):
        pl.semaphore_signal(barrier, inc=1, device_id={"grid": (me + k) % n}, device_id_type=MESH)
    for k in range(1, band_n):
        pl.semaphore_signal(barrier, inc=1, device_id={"band": (band_me + k) % band_n}, device_id_type=MESH)
    pl.semaphore_wait(barrier, n + band_n - 2)

    def start_piece(owner):
        return start.at[0, owner // halves, 0, pl.ds(pl.multiple_of(owner % halves * SUBLANES, SUBLANES), SUBLANES), :]

    def energy_piece(owner):
        return energies.at[owner // halves, pl.ds(pl.multiple_of(owner % halves * SUBLANES, SUBLANES), SUBLANES), :]

    def out_piece(owner):
        return out.at[0, owner // halves, 0, pl.ds(pl.multiple_of(owner % halves * SUBLANES, SUBLANES), SUBLANES), :]

    def spread(piece, landing, send, recv):
        copies = []
        for k in range(1, n):
            peer = (me + k) % n
            copies.append(pltpu.make_async_remote_copy(
                src_ref=piece(peer), dst_ref=landing.at[me], send_sem=send.at[k], recv_sem=recv.at[k],
                device_id={"grid": peer}, device_id_type=MESH))
        own = pltpu.make_async_copy(piece(me), landing.at[me], send.at[0])
        for copy in copies:
            copy.start()
        own.start()
        return copies + [own]

    start_copies = spread(start_piece, got, start_send, start_recv)
    energy_copies = spread(energy_piece, got_energies, energy_send, energy_recv)

    def matrix_rows(y, carry):
        high, low = split(y_table[pl.ds(y, 1), :] * z_table[...])
        at = pl.ds(pl.multiple_of(y * grid_size, grid_size), grid_size)
        mat_high[at, :] = high
        mat_low[at, :] = low
        return carry

    lax.fori_loop(0, grid_size, matrix_rows, 0)
    pot_copy.wait()
    for y in range(grid_size):
        pot_flat[:, y * grid_size:(y + 1) * grid_size] = pot_here[:, y, :]
    table = shifted_potential(pot_flat[...], sites, grid_size) * (1.0 / (grid_size * cells))
    for x in range(grid_size):
        site_table[SUBLANES * x:SUBLANES * (x + 1), :] = jnp.broadcast_to(table[x:x + 1, :], (SUBLANES, cells))
    prev[...] = jnp.zeros_like(prev)
    applied_prev[...] = jnp.zeros_like(prev)

    for copy in start_copies:
        copy.wait()
    for x in range(grid_size):
        at = slice(SUBLANES * x, SUBLANES * (x + 1))
        vec[at, :] = got[x // planes, :, x % planes * cells:(x % planes + 1) * cells]
    vec_high[...], vec_low[...] = split(vec[...])

    blocks = [slice(i, i + block) for i in range(0, cells, block)]
    lane = lax.broadcasted_iota(jnp.int32, (1, LANES), 1)
    tall = 2 * SUBLANES
    zero_sums = (jnp.zeros((SUBLANES, block), jnp.float32),) * 6

    def to_site_and_back():
        x_pair = (x_high[...], x_low[...])
        for cols in blocks:
            mat = (mat_high[:, cols], mat_low[:, cols])
            spectrum = dot3((vec_high[...], vec_low[...]), mat)
            spectrum = dot3(x_pair, split(spectrum)) * site_table[:, cols]
            mid_high[:, cols], mid_low[:, cols] = split(dot3(x_pair, split(spectrum)))

    def finish_apply(source, target):
        for cols in blocks:
            mat = (mat_high[:, cols], mat_low[:, cols])
            target[:, cols] = energy[:, cols] * source[:, cols] - dot3((mid_high[...], mid_low[...]), mat)

    def folded(a, b):
        product = a * b
        return product[:SUBLANES] + product[SUBLANES:]

    def add_moments(sums, here, new, before):
        pairs = ((here, new), (new, new), (here, here), (before, before), (before, new), (here, before))
        return tuple(total + folded(a, b) for total, (a, b) in zip(sums, pairs))

    def message_of(sums):
        message = jnp.zeros((1, LANES), jnp.float32)
        for i in range(6):
            value = jnp.sum(jnp.sum(sums[i], axis=0, keepdims=True), axis=1, keepdims=True)
            message = jnp.where(lane == i, value, message)
        return message

    def exchange(j, message, buffer, axis, size, my, send, recv):
        buffer[j, my] = message
        copies = []
        for k in range(1, size):
            copy = pltpu.make_async_remote_copy(
                src_ref=buffer.at[j, my], dst_ref=buffer.at[j, my], send_sem=send.at[j, k], recv_sem=recv.at[j, k],
                device_id={axis: (my + k) % size}, device_id_type=MESH)
            copy.start()
            copies.append(copy)

        def total():
            for copy in copies:
                copy.wait()
            return jnp.sum(buffer[j], axis=0)

        return total

    def over_grid(j, message):
        return exchange(j, message, grid_sums, "grid", n, me, grid_send, grid_recv)

    def over_band(j, message):
        return exchange(j, message, band_sums, "band", band_n, band_me, band_send, band_recv)

    def coefficients(j, message, beta_prev):
        m = [jnp.sum(jnp.where(lane == i, message, 0.0), axis=1, keepdims=True) / total_count for i in range(6)]
        norm = jnp.where(jnp.full((1, 1), j, jnp.int32) == 0, m[2], 1.0)
        scale = jnp.sqrt(norm)
        alpha = m[0] / norm
        square = m[1] / norm + alpha * alpha * (m[2] / norm) + beta_prev * beta_prev * m[3]
        square = square - 2.0 * alpha * alpha - 2.0 * beta_prev * m[4]
        square = square + 2.0 * alpha * beta_prev * m[5]
        beta = jnp.sqrt(square)
        to_new = 1.0 / (scale * beta)
        return alpha, beta, to_new, alpha * to_new, beta_prev / beta, 1.0 / scale

    def note(j, alpha, beta, alphas, betas):
        return jnp.where(lane == j, alpha, alphas), jnp.where(lane == j, beta, betas)

    def step(j, carry):
        alphas, betas, beta_prev, message = carry
        grid_total = over_grid(j, message)
        to_site_and_back()
        band_total = over_band(j, grid_total())
        finish_apply(applied, twice)
        alpha, beta, to_new, to_here, to_before, to_prev = coefficients(j, band_total(), beta_prev)

        def rows_step(r, sums):
            at = pl.ds(pl.multiple_of(r * tall, tall), tall)
            for cols in blocks:
                here, new, before, applied_before = vec[at, cols], applied[at, cols], prev[at, cols], applied_prev[at, cols]
                vector = to_new * new - to_here * here - to_before * before
                image = to_new * twice[at, cols] - to_here * new - to_before * applied_before
                before = to_prev * here
                vec[at, cols] = vector
                applied[at, cols] = image
                prev[at, cols] = before
                applied_prev[at, cols] = to_prev * new
                vec_high[at, cols], vec_low[at, cols] = split(image)
                sums = add_moments(sums, vector, image, before)
            return sums

        message = message_of(lax.fori_loop(0, rows // tall, rows_step, zero_sums))
        alphas, betas = note(j, alpha, beta, alphas, betas)
        return alphas, betas, beta, message

    to_site_and_back()
    for copy in energy_copies:
        copy.wait()
    for x in range(grid_size):
        at = slice(SUBLANES * x, SUBLANES * (x + 1))
        energy[at, :] = got_energies[x // planes, :, x % planes * cells:(x % planes + 1) * cells]
    finish_apply(vec, applied)

    def first_rows(r, sums):
        at = pl.ds(pl.multiple_of(r * tall, tall), tall)
        for cols in blocks:
            here, new = vec[at, cols], applied[at, cols]
            vec_high[at, cols], vec_low[at, cols] = split(new)
            sums = add_moments(sums, here, new, jnp.zeros_like(here))
        return sums

    message = message_of(lax.fori_loop(0, rows // tall, first_rows, zero_sums))
    zeros = jnp.zeros((1, LANES), jnp.float32)
    carry = (zeros, zeros, jnp.zeros((1, 1), jnp.float32), message)
    last = ITERS - 1
    alphas, betas, beta_prev, message = lax.fori_loop(0, last, step, carry)
    message = over_band(last, over_grid(last, message)())()
    alpha, beta, to_new, to_here, to_before, _ = coefficients(last, message, beta_prev)
    alphas, betas = note(last, alpha, beta, alphas, betas)
    alphas_out[0] = alphas[:, :ITERS]
    betas_out[0] = betas[:, :ITERS]
    for x in range(grid_size):
        at = slice(SUBLANES * x, SUBLANES * (x + 1))
        outgoing[x // planes, :, x % planes * cells:(x % planes + 1) * cells] = (
            to_new * applied[at, :] - to_here * vec[at, :] - to_before * prev[at, :])
    out_copies = []
    for k in range(1, n):
        peer = (me + k) % n
        out_copies.append(pltpu.make_async_remote_copy(
            src_ref=outgoing.at[peer], dst_ref=out_piece(me), send_sem=out_send.at[k], recv_sem=out_recv.at[k],
            device_id={"grid": peer}, device_id_type=MESH))
    out_copies.append(pltpu.make_async_copy(outgoing.at[me], out_piece(me), out_send.at[0]))
    for copy in out_copies:
        copy.start()
    for copy in out_copies:
        copy.wait()


def field_body(start, energies, sites, potential):
    grid_size = potential.shape[0]
    cells = grid_size * grid_size
    n, band_n = lax.axis_size("grid"), lax.axis_size("band")
    halves = start.shape[3] // SUBLANES
    rows = grid_size * SUBLANES
    index = np.arange(grid_size)
    angle = (index[:, None] * index[None, :] % grid_size) * (2.0 * math.pi / grid_size)
    cas = np.cos(angle) + np.sin(angle)
    y_table = jnp.asarray(np.repeat(cas, grid_size, axis=1), jnp.float32)
    z_table = jnp.asarray(np.tile(cas, (1, grid_size)), jnp.float32)
    x_wide = np.kron(cas, np.eye(SUBLANES)).astype(np.float32)
    x_high = x_wide.astype(jnp.bfloat16)
    x_low = (x_wide - x_high.astype(np.float32)).astype(jnp.bfloat16)
    vmem = pl.BlockSpec(memory_space=pltpu.VMEM)
    hbm = pl.BlockSpec(memory_space=pltpu.MemorySpace.HBM)
    slab = (n, SUBLANES, start.shape[4])
    full = pltpu.VMEM((rows, cells), jnp.float32)
    half = pltpu.VMEM((rows, cells), jnp.bfloat16)
    dma = pltpu.SemaphoreType.DMA
    coef = jax.ShapeDtypeStruct((1, 1, ITERS), jnp.float32)
    out, alphas, betas = pl.pallas_call(
        functools.partial(recursion_kernel, (n, band_n, grid_size, halves, min(256, cells))),
        out_shape=(jax.ShapeDtypeStruct(start.shape, jnp.float32), coef, coef),
        in_specs=[hbm, hbm, pl.BlockSpec(memory_space=pltpu.SMEM)] + [hbm] + [vmem] * 4,
        out_specs=(pl.BlockSpec(memory_space=pl.ANY), vmem, vmem),
        scratch_shapes=[
            pltpu.VMEM((grid_size, grid_size, grid_size), jnp.float32), pltpu.VMEM((grid_size, cells), jnp.float32),
            pltpu.VMEM(slab, jnp.float32), pltpu.VMEM(slab, jnp.float32),
            full, full, full, full, full, full, full, half, half, half, half,
            pltpu.VMEM((cells, cells), jnp.bfloat16), pltpu.VMEM((cells, cells), jnp.bfloat16),
            pltpu.VMEM(slab, jnp.float32),
            pltpu.VMEM((ITERS, n, 1, LANES), jnp.float32), pltpu.VMEM((ITERS, band_n, 1, LANES), jnp.float32),
            dma(()), dma((n,)), dma((n,)), dma((n,)), dma((n,)), dma((n,)), dma((n,)),
            dma((ITERS, n)), dma((ITERS, n)), dma((ITERS, band_n)), dma((ITERS, band_n)),
        ],
        compiler_params=pltpu.CompilerParams(collective_id=0, has_side_effects=True, vmem_limit_bytes=50 * 1024 * 1024),
    )(start, energies, sites[:, 0], potential, y_table, z_table, jnp.asarray(x_high), jnp.asarray(x_low))
    return alphas, betas, out


def body(start, energies, sites, potential):
    atoms, cores, pols, bands, _ = start.shape
    grid_size = potential.shape[0]
    whole_fields = (
        atoms == 1 and pols == 1 and bands % SUBLANES == 0
        and cores * bands == SUBLANES * lax.axis_size("grid")
        and grid_size % SUBLANES == 0 and grid_size * grid_size % LANES == 0
    )
    return (field_body if whole_fields else plane_body)(start, energies, sites, potential)


def solution(mesh):
    in_specs = (P(None, None, None, "band", "grid"), P(None, "band", "grid"), P(), P())
    out_specs = (P(), P(), P(None, None, None, "band", "grid"))
    return jax.shard_map(body, mesh=mesh, in_specs=in_specs, out_specs=out_specs, check_vma=False)
```

```python
import functools
import math

import jax
import jax.numpy as jnp
import numpy as np
from jax import lax
from jax.experimental import pallas as pl
from jax.experimental.pallas import tpu as pltpu
from jax.sharding import PartitionSpec as P

ITERS = 4


precise_mode = lax.Precision.HIGHEST


def cas_table(grid_size):
    cells = jnp.arange(grid_size, dtype=jnp.int32)
    phase = cells[:, None] * cells[None, :] % grid_size
    angle = phase.astype(jnp.float32) * (2.0 * math.pi / grid_size)
    return jnp.cos(angle) + jnp.sin(angle)


def shift_axis(field_part, offset, axis_number):
    length = field_part.shape[axis_number]
    doubled = jnp.concatenate([field_part, field_part], axis=axis_number)
    first_index = (length - offset) % length
    return lax.dynamic_slice_in_dim(doubled, first_index, length, axis_number)


def expand_coef(values):
    return values[:, None, :, None, None]


def plane_body(start, energies, sites, potential):
    grid_size = potential.shape[0]
    volume = grid_size * grid_size * grid_size
    atom_count, core_count, pol_count, band_local, kpoint_local = start.shape
    plane_count = grid_size // lax.axis_size("grid")
    position = lax.axis_index("grid")
    chain_count = core_count * pol_count * band_local
    field_count = atom_count * chain_count
    total_count = (
        core_count * band_local * lax.axis_size("band") * kpoint_local * lax.axis_size("grid")
    )
    cas_grid = cas_table(grid_size)
    shifted = shift_axis(potential, sites[0, 0], 0)
    shifted = shift_axis(shifted, sites[1, 0], 1)
    shifted = shift_axis(shifted, sites[2, 0], 2)
    tables = [shifted]
    shifted_all = jnp.stack(tables, axis=-1)
    slab_table = lax.dynamic_slice_in_dim(shifted_all, position * plane_count, plane_count, 1)

    def moment(left, right):
        return jnp.sum(left * right, axis=(1, 3, 4)) / total_count

    start_sum = lax.psum(moment(start, start), ("grid", "band"))
    lanczos = start / expand_coef(jnp.sqrt(start_sum))
    previous = jnp.zeros_like(start)
    beta_prev = jnp.zeros((atom_count, pol_count), jnp.float32)
    alpha_list = []
    beta_list = []
    for iteration in range(ITERS):
        spread_fields = lanczos.reshape(atom_count, chain_count, plane_count, grid_size, grid_size)
        spread_over_z = jnp.einsum(
            "arpyz,wz->pywar", spread_fields, cas_grid, precision=precise_mode
        )
        spread_over_y = jnp.einsum(
            "pywar,uy->puwar", spread_over_z, cas_grid, precision=precise_mode
        )
        direct_spectrum = lax.all_to_all(
            spread_over_y.reshape(plane_count, grid_size, grid_size, field_count),
            "grid",
            split_axis=1,
            concat_axis=0,
            tiled=True,
        )
        field_shape = direct_spectrum.shape
        over_x = jnp.einsum("xvwf,tx->tvwf", direct_spectrum, cas_grid, precision=precise_mode)
        split_view = over_x.reshape(
            field_shape[0], field_shape[1], field_shape[2], atom_count, chain_count
        )
        scaled = split_view * slab_table[..., None]
        back_x = jnp.einsum("tvwar,xt->xvwar", scaled, cas_grid, precision=precise_mode)
        weighted = back_x.reshape(field_shape)
        direct_returned = lax.all_to_all(weighted, "grid", split_axis=0, concat_axis=1, tiled=True)
        fields = direct_returned.reshape(plane_count, grid_size, grid_size, atom_count, chain_count)
        over_z = jnp.einsum("pvwar,zw->pvzar", fields, cas_grid, precision=precise_mode)
        over_y = jnp.einsum("pvzar,yv->arpyz", over_z, cas_grid, precision=precise_mode)
        applied = energies[None, :, None] * lanczos - over_y.reshape(start.shape) / volume
        moments_all = lax.psum(
            (
                moment(lanczos, applied),
                moment(applied, applied),
                moment(lanczos, lanczos),
                moment(previous, previous),
                moment(previous, applied),
                moment(lanczos, previous),
            ),
            ("grid", "band"),
        )
        alpha_now = moments_all[0]
        square = (
            moments_all[1]
            + alpha_now * alpha_now * moments_all[2]
            + beta_prev * beta_prev * moments_all[3]
        )
        square = square - 2.0 * alpha_now * moments_all[0] - 2.0 * beta_prev * moments_all[4]
        square = square + 2.0 * alpha_now * beta_prev * moments_all[5]
        beta_now = jnp.sqrt(square)
        remainder = applied - expand_coef(alpha_now) * lanczos - expand_coef(beta_prev) * previous
        previous = lanczos
        lanczos = remainder / expand_coef(beta_now)
        beta_prev = beta_now
        alpha_list.append(alpha_now)
        beta_list.append(beta_now)
    return (jnp.stack(alpha_list, axis=2), jnp.stack(beta_list, axis=2), lanczos)


MESH = pl.DeviceIdType.MESH
LANES = 128
SUBLANES = 8
WIDE = 1024


def split(value):
    high = value.astype(jnp.bfloat16)
    return high, (value - high.astype(jnp.float32)).astype(jnp.bfloat16)


def dot3(left, right):
    left_high, left_low = left
    right_high, right_low = right
    left = jnp.concatenate([left_high, left_low, left_high], axis=1)
    right = jnp.concatenate([right_high, right_high, right_low], axis=0)
    return jnp.dot(left, right, preferred_element_type=jnp.float32)


def shifted_potential(table, sites, grid_size):
    cells = grid_size * grid_size
    lane = lax.broadcasted_iota(jnp.int32, table.shape, 1) % grid_size
    for axis in range(3):
        step = 1
        while step < grid_size:
            if axis == 0:
                moved = pltpu.roll(table, step, 0)
            elif axis == 1:
                moved = pltpu.roll(table, step * grid_size, 1)
            else:
                moved = jnp.where(
                    lane >= step,
                    pltpu.roll(table, step, 1),
                    pltpu.roll(table, cells - grid_size + step, 1),
                )
            flag = jnp.full(table.shape, sites[axis] // step % 2, jnp.int32)
            table = jnp.where(flag == 1, moved, table)
            step *= 2
    return table


def recursion_kernel(
    sizes, start, energies, sites, pot, y_far, z_far, x_high_far, x_low_far,
    out, coef,
    y_table, z_table, x_high, x_low, pot_here, pot_flat, got, got_energies, vec, prev, applied, applied_prev, twice, energy, site_table, vec_high, vec_low,
    mid_high, mid_low, mat_high, mat_low, outgoing, sums,
    table_sem, start_send, start_recv, energy_send, energy_recv, out_send, out_recv,
    sum_send, sum_recv,
):
    n, band_n, grid_size, halves, block, wide_block = sizes
    me = lax.axis_index("grid")
    rank = lax.axis_index("band") * n + me
    cells = grid_size * grid_size
    planes = grid_size // n
    rows = grid_size * SUBLANES
    total_count = float(rows * cells * n * band_n)

    table_copies = [
        pltpu.make_async_copy(source, target, table_sem.at[i])
        for i, (source, target) in enumerate(((y_far, y_table), (z_far, z_table), (pot, pot_here), (x_high_far, x_high), (x_low_far, x_low)))
    ]
    for copy in table_copies:
        copy.start()
    barrier = pltpu.get_barrier_semaphore()
    for k in range(1, n * band_n):
        peer = (rank + k) % (n * band_n)
        pl.semaphore_signal(barrier, inc=1, device_id={"grid": peer % n, "band": peer // n}, device_id_type=MESH)
    pl.semaphore_wait(barrier, n * band_n - 1)

    def start_piece(owner):
        return start.at[0, owner // halves, 0, pl.ds(pl.multiple_of(owner % halves * SUBLANES, SUBLANES), SUBLANES), :]

    def energy_piece(owner):
        return energies.at[owner // halves, pl.ds(pl.multiple_of(owner % halves * SUBLANES, SUBLANES), SUBLANES), :]

    def out_piece(owner):
        return out.at[0, owner // halves, 0, pl.ds(pl.multiple_of(owner % halves * SUBLANES, SUBLANES), SUBLANES), :]

    def spread(piece, landing, send, recv):
        copies = []
        for k in range(1, n):
            peer = (me + k) % n
            copies.append(pltpu.make_async_remote_copy(
                src_ref=piece(peer), dst_ref=landing.at[me], send_sem=send.at[k], recv_sem=recv.at[k],
                device_id={"grid": peer}, device_id_type=MESH))
        own = pltpu.make_async_copy(piece(me), landing.at[me], send.at[0])
        for copy in copies:
            copy.start()
        own.start()
        return copies + [own]

    start_copies = spread(start_piece, got, start_send, start_recv)
    energy_copies = spread(energy_piece, got_energies, energy_send, energy_recv)

    for copy in table_copies:
        copy.wait()
    def matrix_rows(y, carry):
        high, low = split(y_table[pl.ds(y, 1), :] * z_table[...])
        at = pl.ds(pl.multiple_of(y * grid_size, grid_size), grid_size)
        mat_high[at, :] = high
        mat_low[at, :] = low
        return carry

    lax.fori_loop(0, grid_size, matrix_rows, 0)
    for y in range(grid_size):
        pot_flat[:, y * grid_size:(y + 1) * grid_size] = pot_here[:, y, :]
    table = shifted_potential(pot_flat[...], sites, grid_size) * (1.0 / (grid_size * cells))
    for x in range(grid_size):
        site_table[SUBLANES * x:SUBLANES * (x + 1), :] = jnp.broadcast_to(table[x:x + 1, :], (SUBLANES, cells))
    prev[...] = jnp.zeros_like(prev)
    applied_prev[...] = jnp.zeros_like(prev)

    for copy in start_copies:
        copy.wait()
    for x in range(grid_size):
        at = slice(SUBLANES * x, SUBLANES * (x + 1))
        vec[at, :] = got[x // planes, :, x % planes * cells:(x % planes + 1) * cells]
    vec_high[...], vec_low[...] = split(vec[...])

    blocks = [slice(i, i + block) for i in range(0, cells, block)]
    wide = [slice(i, i + wide_block) for i in range(0, cells, wide_block)]
    lane = lax.broadcasted_iota(jnp.int32, (1, LANES), 1)
    tall = 2 * SUBLANES
    zero_sums = (jnp.zeros((SUBLANES, block), jnp.float32),) * 6

    def to_site_and_back():
        x_pair = (x_high[...], x_low[...])
        for cols in wide:
            mat = (mat_high[:, cols], mat_low[:, cols])
            spectrum = dot3((vec_high[...], vec_low[...]), mat)
            spectrum = dot3(x_pair, split(spectrum)) * site_table[:, cols]
            mid_high[:, cols], mid_low[:, cols] = split(dot3(x_pair, split(spectrum)))

    def finish_apply(source, target):
        for cols in wide:
            mat = (mat_high[:, cols], mat_low[:, cols])
            target[:, cols] = energy[:, cols] * source[:, cols] - dot3((mid_high[...], mid_low[...]), mat)

    def folded(a, b):
        product = a * b
        return product[:SUBLANES] + product[SUBLANES:]

    def add_moments(parts, here, new, before):
        pairs = ((here, new), (new, new), (here, here), (before, before), (before, new), (here, before))
        return tuple(total + folded(a, b) for total, (a, b) in zip(parts, pairs))

    def message_of(parts):
        message = jnp.zeros((1, LANES), jnp.float32)
        for i in range(6):
            value = jnp.sum(jnp.sum(parts[i], axis=0, keepdims=True), axis=1, keepdims=True)
            message = jnp.where(lane == i, value, message)
        return message

    def exchange(j, message):
        sums[j, rank] = message
        copies = []
        for k in range(1, n * band_n):
            peer = (rank + k) % (n * band_n)
            copy = pltpu.make_async_remote_copy(
                src_ref=sums.at[j, rank], dst_ref=sums.at[j, rank], send_sem=sum_send.at[j, k], recv_sem=sum_recv.at[j, k],
                device_id={"grid": peer % n, "band": peer // n}, device_id_type=MESH)
            copy.start()
            copies.append(copy)

        def total():
            for copy in copies:
                copy.wait()
            return jnp.sum(sums[j], axis=0)

        return total

    def coefficients(j, message, beta_prev):
        m = [jnp.sum(jnp.where(lane == i, message, 0.0), axis=1, keepdims=True) / total_count for i in range(6)]
        norm = jnp.where(jnp.full((1, 1), j, jnp.int32) == 0, m[2], 1.0)
        scale = jnp.sqrt(norm)
        alpha = m[0] / norm
        square = m[1] / norm + alpha * alpha * (m[2] / norm) + beta_prev * beta_prev * m[3]
        square = square - 2.0 * alpha * alpha - 2.0 * beta_prev * m[4]
        square = square + 2.0 * alpha * beta_prev * m[5]
        beta = jnp.sqrt(square)
        to_new = 1.0 / (scale * beta)
        return alpha, beta, to_new, alpha * to_new, beta_prev / beta, 1.0 / scale

    def note(j, alpha, beta, alphas, betas):
        return jnp.where(lane == j, alpha, alphas), jnp.where(lane == j, beta, betas)

    def step(j, carry):
        alphas, betas, beta_prev, message = carry
        message_total = exchange(j, message)
        to_site_and_back()
        finish_apply(applied, twice)
        alpha, beta, to_new, to_here, to_before, to_prev = coefficients(j, message_total(), beta_prev)

        def rows_step(r, parts):
            at = pl.ds(pl.multiple_of(r * tall, tall), tall)
            for cols in blocks:
                here, new, before, applied_before = vec[at, cols], applied[at, cols], prev[at, cols], applied_prev[at, cols]
                vector = to_new * new - to_here * here - to_before * before
                image = to_new * twice[at, cols] - to_here * new - to_before * applied_before
                before = to_prev * here
                vec[at, cols] = vector
                applied[at, cols] = image
                prev[at, cols] = before
                applied_prev[at, cols] = to_prev * new
                vec_high[at, cols], vec_low[at, cols] = split(image)
                parts = add_moments(parts, vector, image, before)
            return parts

        message = message_of(lax.fori_loop(0, rows // tall, rows_step, zero_sums))
        alphas, betas = note(j, alpha, beta, alphas, betas)
        return alphas, betas, beta, message

    to_site_and_back()
    for copy in energy_copies:
        copy.wait()
    for x in range(grid_size):
        at = slice(SUBLANES * x, SUBLANES * (x + 1))
        energy[at, :] = got_energies[x // planes, :, x % planes * cells:(x % planes + 1) * cells]
    finish_apply(vec, applied)

    def first_rows(r, parts):
        at = pl.ds(pl.multiple_of(r * tall, tall), tall)
        for cols in blocks:
            here, new = vec[at, cols], applied[at, cols]
            vec_high[at, cols], vec_low[at, cols] = split(new)
            parts = add_moments(parts, here, new, jnp.zeros_like(here))
        return parts

    message = message_of(lax.fori_loop(0, rows // tall, first_rows, zero_sums))
    zeros = jnp.zeros((1, LANES), jnp.float32)
    carry = (zeros, zeros, jnp.zeros((1, 1), jnp.float32), message)
    last = ITERS - 1
    alphas, betas, beta_prev, message = lax.fori_loop(0, last, step, carry)
    message = exchange(last, message)()
    alpha, beta, to_new, to_here, to_before, _ = coefficients(last, message, beta_prev)
    alphas, betas = note(last, alpha, beta, alphas, betas)
    coef[0:1, :] = alphas
    coef[1:2, :] = betas
    out_copies = []
    for k in range(1, n + 1):
        peer = (me + k) % n
        for x in range(planes):
            at = pl.ds(pl.multiple_of((peer * planes + x) * SUBLANES, SUBLANES), SUBLANES)
            outgoing[peer, :, x * cells:(x + 1) * cells] = (
                to_new * applied[at, :] - to_here * vec[at, :] - to_before * prev[at, :])
        if k < n:
            copy = pltpu.make_async_remote_copy(
                src_ref=outgoing.at[peer], dst_ref=out_piece(me), send_sem=out_send.at[k], recv_sem=out_recv.at[k],
                device_id={"grid": peer}, device_id_type=MESH)
        else:
            copy = pltpu.make_async_copy(outgoing.at[me], out_piece(me), out_send.at[0])
        copy.start()
        out_copies.append(copy)
    for copy in out_copies:
        copy.wait()


def field_body(start, energies, sites, potential):
    grid_size = potential.shape[0]
    cells = grid_size * grid_size
    n, band_n = lax.axis_size("grid"), lax.axis_size("band")
    halves = start.shape[3] // SUBLANES
    rows = grid_size * SUBLANES
    index = np.arange(grid_size)
    angle = (index[:, None] * index[None, :] % grid_size) * (2.0 * math.pi / grid_size)
    cas = np.cos(angle) + np.sin(angle)
    y_table = jnp.asarray(np.repeat(cas, grid_size, axis=1), jnp.float32)
    z_table = jnp.asarray(np.tile(cas, (1, grid_size)), jnp.float32)
    x_wide = np.kron(cas, np.eye(SUBLANES)).astype(np.float32)
    x_high = x_wide.astype(jnp.bfloat16)
    x_low = (x_wide - x_high.astype(np.float32)).astype(jnp.bfloat16)
    vmem = pl.BlockSpec(memory_space=pltpu.VMEM)
    hbm = pl.BlockSpec(memory_space=pltpu.MemorySpace.HBM)
    slab = (n, SUBLANES, start.shape[4])
    full = pltpu.VMEM((rows, cells), jnp.float32)
    half = pltpu.VMEM((rows, cells), jnp.bfloat16)
    dma = pltpu.SemaphoreType.DMA
    out, coef = pl.pallas_call(
        functools.partial(recursion_kernel, (n, band_n, grid_size, halves, min(256, cells), min(WIDE, cells))),
        out_shape=(jax.ShapeDtypeStruct(start.shape, jnp.float32), jax.ShapeDtypeStruct((2, LANES), jnp.float32)),
        in_specs=[hbm, hbm, pl.BlockSpec(memory_space=pltpu.SMEM)] + [hbm] * 5,
        out_specs=(vmem, vmem),
        scratch_shapes=[
            pltpu.VMEM((grid_size, cells), jnp.float32), pltpu.VMEM((grid_size, cells), jnp.float32),
            pltpu.VMEM((rows, rows), jnp.bfloat16), pltpu.VMEM((rows, rows), jnp.bfloat16),
            pltpu.VMEM((grid_size, grid_size, grid_size), jnp.float32), pltpu.VMEM((grid_size, cells), jnp.float32),
            pltpu.VMEM(slab, jnp.float32), pltpu.VMEM(slab, jnp.float32),
            full, full, full, full, full, full, full, half, half, half, half,
            pltpu.VMEM((cells, cells), jnp.bfloat16), pltpu.VMEM((cells, cells), jnp.bfloat16),
            pltpu.VMEM(slab, jnp.float32),
            pltpu.VMEM((ITERS, n * band_n, 1, LANES), jnp.float32),
            dma((5,)), dma((n,)), dma((n,)), dma((n,)), dma((n,)), dma((n,)), dma((n,)),
            dma((ITERS, n * band_n)), dma((ITERS, n * band_n)),
        ],
        compiler_params=pltpu.CompilerParams(collective_id=0, has_side_effects=True, vmem_limit_bytes=60 * 1024 * 1024),
    )(start, energies, sites[:, 0], potential, y_table, z_table, jnp.asarray(x_high), jnp.asarray(x_low))
    return coef[0, :ITERS].reshape(1, 1, ITERS), coef[1, :ITERS].reshape(1, 1, ITERS), out


def body(start, energies, sites, potential):
    atoms, cores, pols, bands, _ = start.shape
    grid_size = potential.shape[0]
    whole_fields = (
        atoms == 1 and pols == 1 and bands % SUBLANES == 0
        and cores * bands == SUBLANES * lax.axis_size("grid")
        and grid_size % SUBLANES == 0 and grid_size * grid_size % LANES == 0
    )
    return (field_body if whole_fields else plane_body)(start, energies, sites, potential)


def solution(mesh):
    in_specs = (P(None, None, None, "band", "grid"), P(None, "band", "grid"), P(), P())
    out_specs = (P(), P(), P(None, None, None, "band", "grid"))
    return jax.shard_map(body, mesh=mesh, in_specs=in_specs, out_specs=out_specs, check_vma=False)
```
